256 devices in a mesh: loader: 64 (over z, x, core), split: 4 (over y).
Axes of the slice: x: 4, y: 4, z: 8, core: 2. Of those that a mesh axis runs over, the one named last changes fastest.
Arguments:
- embeddings: bfloat16 [131072, 768], P(('loader', 'split')), may hold values from -6 to 6
- cluster_ids: int32 [131072, 1], P(('loader', 'split')), may hold values from 0 to 255; in each aligned block of 512 rows (0 to 511, 512 to 1023, ...) at most 4 rows name the same one
- ranks: int32 [131072], P(('loader', 'split')), may hold values from 0 to 131071, each once
Outputs:
- nearest: float32 [131072], P(('loader', 'split'))
The draws below stay inside these ranges and needn't reach their ends.
Inputs may be any that keep to these rules, and one draw needn't show every extreme that they name: `cluster_ids`: among the 512 rows of one device no cluster appears more than 4 times. All ranks differ.
All inputs are finite; a program needn't handle non-finite values.
Results may differ from the reference program's by a relative error of at most 0.0014.
Values may be sent and summed in bfloat16 or wider, within the bound.
No kernel may reach another device: no remote copies, remote signals or barrier semaphores. Data moves between devices by JAX's collectives and lax.ppermute only.
A program may use at most 64 MiB of HBM per device.

```python
import math
import jax
import jax.numpy as jnp
import numpy as np
from jax import lax

D = 768
ROWS_DEV = 512
CLUSTERS = 256
CAP = 4
ROWS = 131072
WINDOW = 1024


def steps_of(stream_key, extent, cuts, least, largest):
    factor_of, own = 1.0, jax.random.fold_in(stream_key, 6)
    for dim, parts in cuts:
        steps = jnp.exp(jax.random.uniform(jax.random.fold_in(own, dim), (parts,), jnp.float32, least / len(cuts), largest / len(cuts)))
        factor_of = factor_of * jnp.repeat(steps, extent[dim] // parts).reshape([-1 if axis == dim else 1 for axis in range(len(extent))])
    return factor_of


def routed_block(stream_key, own, number, rows, count, top, limit, skew):
    order = jax.random.permutation(stream_key, count)
    crowded, common = load_shares(count, rows * top, limit, skew, True), load_shares(count, rows * top, limit, skew, False)
    places = jnp.arange(count)

    def named(lengths, turn):
        used = int((lengths > 0).sum())
        fixed = max(1, used // 4)
        shifted = fixed + (places - fixed + turn * (used - fixed)) % max(1, count - fixed)
        return jnp.zeros((count,), jnp.int32).at[order[jnp.where(places < fixed, places, shifted)]].set(jnp.asarray(lengths, jnp.int32))

    lengths = jnp.where(number % 4 == 0, named(crowded, number // 4), named(common, number - number // 4 - 1))
    mixed = jax.random.permutation(jax.random.fold_in(own, 3), count)
    giver, taker = mixed[0:count // 2 * 2:2], mixed[1:count // 2 * 2:2]
    margin = jnp.minimum(lengths[giver] - 1, limit - lengths[taker]) // 2
    margin = jnp.where((giver == order[0]) | (taker == order[0]) | (lengths[taker] == 0), 0, jnp.maximum(margin, 0))
    shifted = jax.random.randint(jax.random.fold_in(own, 4), (count // 2,), 0, 1 << 20) % (margin + 1)
    lengths = lengths.at[giver].add(-shifted).at[taker].add(shifted)
    items = jnp.searchsorted(jnp.cumsum(lengths), jnp.arange(rows * top), side="right").astype(jnp.int32)
    grid = items.reshape(top, rows).T
    grid = grid[jax.random.permutation(jax.random.fold_in(own, 1), rows)]
    turn = jax.random.randint(jax.random.fold_in(own, 2), (rows, 1), 0, top)
    return jnp.take_along_axis(grid, (jnp.arange(top)[None, :] + turn) % top, axis=1)


def load_shares(amount, total, most, lean, full):
    portions = [(1 << 20) // math.isqrt(standing ** lean) + 1 for standing in range(1, amount + 1)]
    largest = most if full else min(most, max(-(-total // amount), total * portions[0] // sum(portions)))
    least = 1 if total - largest >= amount - 1 else 0
    given, surplus = [largest] + [least] * (amount - 1), total - largest - least * (amount - 1)
    while surplus > 0:
        movable = [i for i in range(1, amount) if given[i] < largest] or [i for i in range(1, amount) if given[i] < most]
        whole, left = sum([portions[i] for i in movable]), surplus
        for i in movable:
            addition = min(most - given[i], max(1, left * portions[i] // whole), surplus)
            given[i] = given[i] + addition
            surplus = surplus - addition
    return np.array(given)


def scatter_about(own_key, dims, scale, limit, cuts=(), kind=jnp.bfloat16):
    entries = jax.random.normal(own_key, dims, jnp.float32) * scale
    if len(cuts) > 0:
        entries = steps_of(own_key, dims, cuts, -0.22, 0.18) * entries
    return jnp.clip(entries, min=-limit, max=limit).astype(kind)


def setup_inputs(seed: int = 0) -> dict:
    keys = jax.random.split(jax.random.key(seed), 4)
    embeddings = scatter_about(keys[0], (ROWS, D), 1.0, 6.0, ((0, 256),))
    cluster_ids_keys = jax.random.split(jax.random.fold_in(keys[1], 1), ROWS // ROWS_DEV)
    cluster_ids_turns = jax.random.permutation(jax.random.fold_in(keys[1], 3), ROWS // ROWS_DEV)
    cluster_ids = jax.vmap(lambda own, number: routed_block(jax.random.fold_in(keys[1], 2), own, number, ROWS_DEV, CLUSTERS, 1, CAP, 2))(cluster_ids_keys, cluster_ids_turns).reshape((ROWS, 1))
    ranks = jax.random.permutation(keys[2], ROWS).astype(jnp.int32)
    return dict(embeddings=embeddings, cluster_ids=cluster_ids, ranks=ranks)


epsilon = 1e-06

def reference(embeddings, cluster_ids, ranks):
    values = embeddings.astype(jnp.float32)
    unit = (values * lax.rsqrt(lax.optimization_barrier(jnp.sum(values * values, axis=1, keepdims=True)) + epsilon)).astype(jnp.bfloat16)
    cluster = cluster_ids[:, 0].astype(jnp.int32)
    row_order = jnp.argsort(cluster, stable=True).astype(jnp.int32)
    sorted_cluster = cluster[row_order]
    sorted_unit = unit[row_order]
    sorted_rank = ranks[row_order]
    offsets = jnp.searchsorted(sorted_cluster, jnp.arange(CLUSTERS, dtype=jnp.int32)).astype(jnp.int32)
    padded_unit = jnp.concatenate([sorted_unit, jnp.zeros((WINDOW, unit.shape[1]), jnp.bfloat16)], axis=0)
    padded_cluster = jnp.concatenate([sorted_cluster, jnp.full((WINDOW,), -1, jnp.int32)], axis=0)
    padded_rank = jnp.concatenate([sorted_rank, jnp.full((WINDOW,), -1, jnp.int32)], axis=0)

    def per_cluster(which):
        offset = offsets[which]
        members = lax.dynamic_slice_in_dim(padded_unit, offset, WINDOW, 0)
        member_cluster = lax.dynamic_slice_in_dim(padded_cluster, offset, WINDOW, 0)
        member_rank = lax.dynamic_slice_in_dim(padded_rank, offset, WINDOW, 0)
        scores = jnp.dot(members, members.T, preferred_element_type=jnp.float32)
        allowed = (member_cluster == which)[None, :] & (member_rank[None, :] < member_rank[:, None])
        return lax.optimization_barrier(jnp.max(jnp.where(allowed, scores, jnp.float32(-1.0)), axis=1))
    results = lax.map(per_cluster, jnp.arange(CLUSTERS, dtype=jnp.int32))
    position = jnp.arange(sorted_cluster.shape[0], dtype=jnp.int32) - offsets[sorted_cluster]
    sorted_result = results[sorted_cluster, position]
    return jnp.zeros((cluster.shape[0],), jnp.float32).at[row_order].set(sorted_result)
```

```python
import jax
import jax.numpy as jnp
from jax import lax
from jax.experimental import pallas as pl
from jax.experimental.pallas import tpu as pltpu
from jax.sharding import PartitionSpec as P

CLUSTERS = 256
CAP = 4
LANES = 128
BLOCKS = 4
DIGIT = 64
AXES = ("loader", "split")
VMEM = pl.BlockSpec(memory_space=pltpu.VMEM)

epsilon = 1e-06


def iota(dims, dim):
    return lax.broadcasted_iota(jnp.int32, dims, dim)


def flag(mask):
    return mask.astype(jnp.float32).astype(jnp.bfloat16)


def dot(a, b, contract_b=0):
    return lax.dot_general(
        a, b, (((1,), (contract_b,)), ((), ())), preferred_element_type=jnp.float32
    )


def pack(ids_ref, rank_ref, rows_ref, out_ref, target_ref, held, unit_ref, digit_ref, slot_ref, sem):
    rows, width = held.shape
    step = pl.program_id(0)

    @pl.when(step == 0)
    def prepare():
        load = pltpu.make_async_copy(rows_ref, held, sem)
        load.start()
        cluster = ids_ref[...]
        member = iota((CLUSTERS, rows), 0) == cluster
        before = iota((rows, rows), 0) < iota((rows, rows), 1)
        count = dot(flag(member), flag(before))
        position = jnp.sum(jnp.where(member, count, 0.0), axis=0, keepdims=True).astype(jnp.int32)
        target = cluster * CAP + position
        target_ref[...] = target
        slot_ref[...] = target
        rank = rank_ref[...] + 1
        which = iota((LANES, rows), 0)
        high, middle, low = rank // (DIGIT * DIGIT), rank // DIGIT % DIGIT, rank % DIGIT
        which = jnp.where(which >= 3, which - 3, which)
        digits = jnp.where(which == 0, high, jnp.where(which == 1, middle, jnp.where(which == 2, low, 0)))
        digit_ref[...] = digits.astype(jnp.float32).astype(jnp.bfloat16)
        load.wait()
        values = held[...].astype(jnp.float32)
        scale = lax.rsqrt(jnp.sum(values * values, axis=1, keepdims=True) + epsilon)
        unit_ref[...] = (values * scale).astype(jnp.bfloat16)

    owners = CLUSTERS // BLOCKS
    pairs = owners * 2
    target = slot_ref[...]
    local = iota((pairs, rows), 0)
    wanted = (local // 2 + step * owners) * CAP + local % 2
    pick = jnp.concatenate([flag(wanted == target), flag(wanted + 2 == target)], axis=0)
    packed = dot(pick, unit_ref[...]).astype(jnp.bfloat16)
    out_ref[:, :, :width] = packed[:pairs].reshape(owners, 2, width)
    out_ref[:, :, width : 2 * width] = packed[pairs:].reshape(owners, 2, width)
    digits = dot(pick, digit_ref[...], 1)
    digits = jnp.where(iota((pairs, LANES), 1) < 3, digits[:pairs], digits[pairs:])
    out_ref[:, :, 2 * width :] = digits.astype(jnp.bfloat16).reshape(owners, 2, LANES)


def score(rows_ref, out_ref, keys_ref, best_ref):
    sources, _, wide = rows_ref.shape
    slots, width = keys_ref.shape
    half = slots // 2
    block = 256
    keys_ref[:half, :] = rows_ref[:, :, :width].reshape(half, width)
    keys_ref[half:, :] = rows_ref[:, :, width : 2 * width].reshape(half, width)
    digits = rows_ref[:, :, 2 * width :].reshape(half, LANES)
    def weights(dims, dim, other, size):
        place = iota(dims, dim) - 3 * (iota(dims, other) // size)
        value = jnp.where(place == 0, DIGIT * DIGIT, jnp.where(place == 1, DIGIT, jnp.where(place == 2, 1, 0)))
        return value.astype(jnp.float32).astype(jnp.bfloat16)
    column = dot(digits, weights((LANES, 2 * LANES), 0, 1, LANES))
    row = dot(weights((8, LANES), 1, 0, 1), digits, 1)
    row = jnp.where(row == 0.0, 1e9, row)
    keys = keys_ref[...]
    for q in range(slots // block):
        scores = dot(keys_ref[q * block : (q + 1) * block, :], keys, 1)
        side, start = divmod(q * block, half)
        query_rank = column[start : start + block, side * LANES : (side + 1) * LANES]
        best = jnp.full((block, LANES), -1.0, jnp.float32)
        for k in range(slots // LANES):
            part = k * LANES
            key_rank = row[part // half : part // half + 1, part % half : part % half + LANES]
            allowed = key_rank < query_rank
            best = jnp.maximum(best, jnp.where(allowed, scores[:, part : part + LANES], -1.0))
        best_ref[q * block : (q + 1) * block, :] = jnp.broadcast_to(
            jnp.max(best, axis=1, keepdims=True), (block, LANES)
        )
    lane = iota((sources, LANES), 1)
    out = best_ref[pl.ds(0, sources, stride=2), :]
    for p in range(1, CAP):
        start = p // 2 * half + p % 2
        out = jnp.where(lane == p, best_ref[pl.ds(start, sources, stride=2), :], out)
    out_ref[...] = out


def unpack(back_ref, target_ref, out_ref):
    rows = target_ref.shape[1]
    back = back_ref[...]
    target = target_ref[...]
    position = target % CAP
    value = jnp.broadcast_to(back[:, 0:1], (CLUSTERS, rows))
    for p in range(1, CAP):
        value = jnp.where(position == p, jnp.broadcast_to(back[:, p : p + 1], (CLUSTERS, rows)), value)
    member = iota((CLUSTERS, rows), 0) == target // CAP
    out_ref[...] = jnp.sum(jnp.where(member, value, 0.0), axis=0, keepdims=True)


def on_chip(x):
    return pltpu.with_memory_space_constraint(x, pltpu.VMEM)


def exchange(x):
    return lax.all_to_all(x, AXES, 0, 0, tiled=True)


def shards(embeddings, cluster_ids, ranks):
    rows, width = embeddings.shape
    slots = CLUSTERS * CAP
    wide = 2 * width + LANES
    f32, i32, bf16 = jnp.float32, jnp.int32, jnp.bfloat16
    shape = jax.ShapeDtypeStruct
    whole = lambda dims: pl.BlockSpec(dims, lambda i: (0,) * len(dims))
    packed, target = pl.pallas_call(
        pack,
        grid=(BLOCKS,),
        out_shape=(shape((CLUSTERS, 2, wide), bf16), shape((1, rows), i32)),
        in_specs=[whole((1, rows)), whole((1, rows)), pl.BlockSpec(memory_space=pl.ANY)],
        out_specs=(
            pl.BlockSpec((CLUSTERS // BLOCKS, 2, wide), lambda i: (i, 0, 0)),
            whole((1, rows)),
        ),
        scratch_shapes=[
            pltpu.VMEM((rows, width), bf16),
            pltpu.VMEM((rows, width), bf16),
            pltpu.VMEM((LANES, rows), bf16),
            pltpu.VMEM((1, rows), i32),
            pltpu.SemaphoreType.DMA,
        ],
        name="pack",
    )(cluster_ids.reshape(1, rows), ranks.reshape(1, rows), embeddings)
    arrived = exchange(packed)
    best = pl.pallas_call(
        score,
        out_shape=pltpu.VMEM((CLUSTERS, LANES), f32),
        in_specs=[VMEM],
        out_specs=VMEM,
        scratch_shapes=[pltpu.VMEM((slots, width), bf16), pltpu.VMEM((slots, LANES), f32)],
        name="score",
    )(on_chip(arrived))
    back = exchange(best.reshape(CLUSTERS, 1, LANES)).reshape(CLUSTERS, LANES)
    out = pl.pallas_call(
        unpack, out_shape=shape((1, rows), f32), in_specs=[VMEM, VMEM], name="unpack"
    )(on_chip(back), target)
    return out.reshape(rows)


def solution(mesh):
    return jax.shard_map(
        shards,
        mesh=mesh,
        in_specs=(P(AXES, None), P(AXES, None), P(AXES)),
        out_specs=P(AXES),
        check_vma=False,
    )
```

```python
import jax
import jax.numpy as jnp
from jax import lax
from jax.experimental import pallas as pl
from jax.experimental.pallas import tpu as pltpu
from jax.sharding import PartitionSpec as P

CLUSTERS = 256
CAP = 4
LANES = 128
BLOCKS = 4
CHUNKS = 4
DIGIT = 64
AXES = ("loader", "split")
VMEM = pl.BlockSpec(memory_space=pltpu.VMEM)

epsilon = 1e-06


def iota(dims, dim):
    return lax.broadcasted_iota(jnp.int32, dims, dim)


def flag(mask):
    return mask.astype(jnp.float32).astype(jnp.bfloat16)


def dot(a, b, contract_b=0):
    return lax.dot_general(
        a, b, (((1,), (contract_b,)), ((), ())), preferred_element_type=jnp.float32
    )


def pack(ids_hbm, rank_hbm, rows_hbm, out_ref, target_ref, ids_ref, rank_ref, held, unit_ref, digit_ref, sems):
    rows, width = held.shape
    chunk = rows // CHUNKS
    loads = [pltpu.make_async_copy(ids_hbm, ids_ref, sems.at[0]), pltpu.make_async_copy(rank_hbm, rank_ref, sems.at[1])]
    for c in range(CHUNKS):
        part = pl.ds(c * chunk, chunk)
        loads.append(pltpu.make_async_copy(rows_hbm.at[part], held.at[part], sems.at[2 + c]))
    for load in loads:
        load.start()
    loads[0].wait()
    loads[1].wait()
    cluster = ids_ref[...]
    member = iota((CLUSTERS, rows), 0) == cluster
    before = iota((rows, rows), 0) < iota((rows, rows), 1)
    count = dot(flag(member), flag(before))
    position = jnp.sum(jnp.where(member, count, 0.0), axis=0, keepdims=True).astype(jnp.int32)
    target = cluster * CAP + position
    target_ref[...] = target
    rank = rank_ref[...] + 1
    which = iota((LANES, rows), 0)
    which = jnp.where(which >= 3, which - 3, which)
    high, middle, low = rank // (DIGIT * DIGIT), rank // DIGIT % DIGIT, rank % DIGIT
    digits = jnp.where(which == 0, high, jnp.where(which == 1, middle, jnp.where(which == 2, low, 0)))
    digit_ref[...] = digits.astype(jnp.float32).astype(jnp.bfloat16)
    for c in range(CHUNKS):
        loads[2 + c].wait()
        values = held[c * chunk : (c + 1) * chunk, :].astype(jnp.float32)
        scale = lax.rsqrt(jnp.sum(values * values, axis=1, keepdims=True) + epsilon)
        unit_ref[c * chunk : (c + 1) * chunk, :] = (values * scale).astype(jnp.bfloat16)
    owners = CLUSTERS // BLOCKS
    pairs = owners * 2
    local = iota((pairs, rows), 0)
    local = local // 2 * CAP + local % 2
    for step in range(BLOCKS):
        wanted = local + step * owners * CAP
        pick = jnp.concatenate([flag(wanted == target), flag(wanted + 2 == target)], axis=0)
        packed = dot(pick, unit_ref[...]).astype(jnp.bfloat16)
        out = out_ref.at[step * owners : (step + 1) * owners]
        out[:, :, :width] = packed[:pairs].reshape(owners, 2, width)
        out[:, :, width : 2 * width] = packed[pairs:].reshape(owners, 2, width)
        digits = dot(pick, digit_ref[...], 1)
        digits = jnp.where(iota((pairs, LANES), 1) < 3, digits[:pairs], digits[pairs:])
        out[:, :, 2 * width :] = digits.astype(jnp.bfloat16).reshape(owners, 2, LANES)


def score(rows_ref, out_ref, keys_ref, best_ref):
    sources, _, wide = rows_ref.shape
    slots, width = keys_ref.shape
    half = slots // 2
    block = 256
    keys_ref[:half, :] = rows_ref[:, :, :width].reshape(half, width)
    keys_ref[half:, :] = rows_ref[:, :, width : 2 * width].reshape(half, width)
    digits = rows_ref[:, :, 2 * width :].reshape(half, LANES)
    def weights(dims, dim, other, size):
        place = iota(dims, dim) - 3 * (iota(dims, other) // size)
        value = jnp.where(place == 0, DIGIT * DIGIT, jnp.where(place == 1, DIGIT, jnp.where(place == 2, 1, 0)))
        return value.astype(jnp.float32).astype(jnp.bfloat16)
    column = dot(digits, weights((LANES, 2 * LANES), 0, 1, LANES))
    row = dot(weights((8, LANES), 1, 0, 1), digits, 1)
    row = jnp.where(row == 0.0, 1e9, row)
    keys = keys_ref[...]
    for q in range(slots // block):
        scores = dot(keys_ref[q * block : (q + 1) * block, :], keys, 1)
        side, start = divmod(q * block, half)
        query_rank = column[start : start + block, side * LANES : (side + 1) * LANES]
        best = jnp.full((block, LANES), -1.0, jnp.float32)
        for k in range(slots // LANES):
            part = k * LANES
            key_rank = row[part // half : part // half + 1, part % half : part % half + LANES]
            allowed = key_rank < query_rank
            best = jnp.maximum(best, jnp.where(allowed, scores[:, part : part + LANES], -1.0))
        best_ref[q * block : (q + 1) * block, :] = jnp.broadcast_to(
            jnp.max(best, axis=1, keepdims=True), (block, LANES)
        )
    lane = iota((sources, LANES), 1)
    out = best_ref[pl.ds(0, sources, stride=2), :]
    for p in range(1, CAP):
        start = p // 2 * half + p % 2
        out = jnp.where(lane == p, best_ref[pl.ds(start, sources, stride=2), :], out)
    out_ref[...] = out


def unpack(back_ref, target_ref, out_ref):
    rows = target_ref.shape[1]
    back = back_ref[...]
    target = target_ref[...]
    position = target % CAP
    value = jnp.broadcast_to(back[:, 0:1], (CLUSTERS, rows))
    for p in range(1, CAP):
        value = jnp.where(position == p, jnp.broadcast_to(back[:, p : p + 1], (CLUSTERS, rows)), value)
    member = iota((CLUSTERS, rows), 0) == target // CAP
    out_ref[...] = jnp.sum(jnp.where(member, value, 0.0), axis=0, keepdims=True)


def on_chip(x):
    return pltpu.with_memory_space_constraint(x, pltpu.VMEM)


def exchange(x):
    return lax.all_to_all(x, AXES, 0, 0, tiled=True)


def shards(embeddings, cluster_ids, ranks):
    rows, width = embeddings.shape
    slots = CLUSTERS * CAP
    wide = 2 * width + LANES
    f32, i32, bf16 = jnp.float32, jnp.int32, jnp.bfloat16
    shape = jax.ShapeDtypeStruct
    packed, target = pl.pallas_call(
        pack,
        out_shape=(pltpu.VMEM((CLUSTERS, 2, wide), bf16), pltpu.VMEM((1, rows), i32)),
        in_specs=[pl.BlockSpec(memory_space=pl.ANY)] * 3,
        out_specs=(VMEM, VMEM),
        scratch_shapes=[
            pltpu.VMEM((1, rows), i32),
            pltpu.VMEM((1, rows), i32),
            pltpu.VMEM((rows, width), bf16),
            pltpu.VMEM((rows, width), bf16),
            pltpu.VMEM((LANES, rows), bf16),
            pltpu.SemaphoreType.DMA((2 + CHUNKS,)),
        ],
        name="pack",
    )(cluster_ids.reshape(1, rows), ranks.reshape(1, rows), embeddings)
    arrived = exchange(packed)
    best = pl.pallas_call(
        score,
        out_shape=pltpu.VMEM((CLUSTERS, LANES), f32),
        in_specs=[VMEM],
        out_specs=VMEM,
        scratch_shapes=[pltpu.VMEM((slots, width), bf16), pltpu.VMEM((slots, LANES), f32)],
        name="score",
    )(on_chip(arrived))
    back = exchange(best.reshape(CLUSTERS, 1, LANES)).reshape(CLUSTERS, LANES)
    out = pl.pallas_call(
        unpack, out_shape=shape((1, rows), f32), in_specs=[VMEM, VMEM], name="unpack"
    )(on_chip(back), on_chip(target))
    return out.reshape(rows)


def solution(mesh):
    return jax.shard_map(
        shards,
        mesh=mesh,
        in_specs=(P(AXES, None), P(AXES, None), P(AXES)),
        out_specs=P(AXES),
        check_vma=False,
    )
```

```python
import jax
import jax.numpy as jnp
from jax import lax
from jax.experimental import pallas as pl
from jax.experimental.pallas import tpu as pltpu
from jax.sharding import PartitionSpec as P

CLUSTERS = 256
CAP = 4
LANES = 128
BLOCKS = 4
CHUNKS = 2
DIGIT = 64
TILE = 256
AXES = ("loader", "split")
VMEM = pl.BlockSpec(memory_space=pltpu.VMEM)

epsilon = 1e-06


def iota(dims, dim):
    return lax.broadcasted_iota(jnp.int32, dims, dim)


def flag(mask):
    return mask.astype(jnp.float32).astype(jnp.bfloat16)


def dot(a, b, contract_b=0):
    return lax.dot_general(
        a, b, (((1,), (contract_b,)), ((), ())), preferred_element_type=jnp.float32
    )


def pack(ids_hbm, rank_hbm, rows_hbm, out_ref, target_ref, ids_ref, rank_ref, held, unit_ref, digit_ref, sems):
    rows, width = held.shape
    chunk = rows // CHUNKS
    loads = [pltpu.make_async_copy(ids_hbm, ids_ref, sems.at[0]), pltpu.make_async_copy(rank_hbm, rank_ref, sems.at[1])]
    for c in range(CHUNKS):
        part = pl.ds(c * chunk, chunk)
        loads.append(pltpu.make_async_copy(rows_hbm.at[part], held.at[part], sems.at[2 + c]))
    for load in loads:
        load.start()
    loads[0].wait()
    loads[1].wait()
    cluster = ids_ref[...]
    member = iota((CLUSTERS, rows), 0) == cluster
    before = iota((rows, rows), 0) < iota((rows, rows), 1)
    count = dot(flag(member), flag(before))
    position = jnp.sum(jnp.where(member, count, 0.0), axis=0, keepdims=True).astype(jnp.int32)
    target = cluster * CAP + position
    target_ref[...] = target
    rank = rank_ref[...] + 1
    which = iota((LANES, rows), 0)
    which = jnp.where(which >= 3, which - 3, which)
    high, middle, low = rank // (DIGIT * DIGIT), rank // DIGIT % DIGIT, rank % DIGIT
    digits = jnp.where(which == 0, high, jnp.where(which == 1, middle, jnp.where(which == 2, low, 0)))
    digit_ref[...] = digits.astype(jnp.float32).astype(jnp.bfloat16)
    for c in range(CHUNKS):
        loads[2 + c].wait()
        values = held[c * chunk : (c + 1) * chunk, :].astype(jnp.float32)
        scale = lax.rsqrt(jnp.sum(values * values, axis=1, keepdims=True) + epsilon)
        unit_ref[c * chunk : (c + 1) * chunk, :] = (values * scale).astype(jnp.bfloat16)
    owners = CLUSTERS // BLOCKS
    pairs = owners * 2
    local = iota((pairs, rows), 0)
    local = local // 2 * CAP + local % 2
    for step in range(BLOCKS):
        wanted = local + step * owners * CAP
        pick = jnp.concatenate([flag(wanted == target), flag(wanted + 2 == target)], axis=0)
        packed = dot(pick, unit_ref[...]).astype(jnp.bfloat16)
        out = out_ref.at[step * owners : (step + 1) * owners]
        out[:, :, :width] = packed[:pairs].reshape(owners, 2, width)
        out[:, :, width : 2 * width] = packed[pairs:].reshape(owners, 2, width)
        digits = dot(pick, digit_ref[...], 1)
        digits = jnp.where(iota((pairs, LANES), 1) < 3, digits[:pairs], digits[pairs:])
        out[:, :, 2 * width :] = digits.astype(jnp.bfloat16).reshape(owners, 2, LANES)


def score(rows_ref, out_ref, keys_ref, best_ref):
    sources, _, wide = rows_ref.shape
    slots, width = keys_ref.shape
    half = slots // 2
    keys_ref[:half, :] = rows_ref[:, :, :width].reshape(half, width)
    keys_ref[half:, :] = rows_ref[:, :, width : 2 * width].reshape(half, width)
    digits = rows_ref[:, :, 2 * width :].reshape(half, LANES)

    def weights(dims, dim, other, size):
        place = iota(dims, dim) - 3 * (iota(dims, other) // size)
        value = jnp.where(place == 0, DIGIT * DIGIT, jnp.where(place == 1, DIGIT, jnp.where(place == 2, 1, 0)))
        return value.astype(jnp.float32).astype(jnp.bfloat16)

    def settled(rank):
        return jnp.where(rank == 0.0, 1e9, rank)

    column = settled(dot(digits, weights((LANES, 2 * LANES), 0, 1, LANES)))
    row = settled(dot(weights((8, LANES), 1, 0, 1), digits, 1))
    count = slots // TILE
    parts = TILE // LANES

    def down(block):
        side, start = divmod(block * TILE, half)
        return column[start : start + TILE, side * LANES : (side + 1) * LANES]

    def across(block, part):
        side, start = divmod(block * TILE + part * LANES, half)
        return row[side : side + 1, start : start + LANES]

    diagonal = iota((LANES, LANES), 0) == iota((LANES, LANES), 1)
    best = [jnp.full((TILE, LANES), -1.0, jnp.float32)] * count
    for j in range(count):
        top = [jnp.full((8, LANES), -1.0, jnp.float32)] * parts
        for i in range(j + 1):
            scores = dot(keys_ref[i * TILE : (i + 1) * TILE, :], keys_ref[j * TILE : (j + 1) * TILE, :], 1)
            for part in range(parts):
                piece = scores[:, part * LANES : (part + 1) * LANES]
                allowed = across(j, part) < down(i)
                best[i] = jnp.maximum(best[i], jnp.where(allowed, piece, -1.0))
                if i < j:
                    other = jnp.where(allowed, -1.0, piece).reshape(TILE // 8, 8, LANES)
                    top[part] = jnp.maximum(top[part], jnp.max(other, axis=0))
        if j > 0:
            extra = [
                jnp.where(diagonal, jnp.max(top[part], axis=0, keepdims=True), -1.0)
                for part in range(parts)
            ]
            best[j] = jnp.maximum(best[j], jnp.concatenate(extra, axis=0))
    for i in range(count):
        best_ref[i * TILE : (i + 1) * TILE, :] = jnp.broadcast_to(
            jnp.max(best[i], axis=1, keepdims=True), (TILE, LANES)
        )
    lane = iota((sources, LANES), 1)
    out = best_ref[pl.ds(0, sources, stride=2), :]
    for p in range(1, CAP):
        start = p // 2 * half + p % 2
        out = jnp.where(lane == p, best_ref[pl.ds(start, sources, stride=2), :], out)
    out_ref[...] = out


def unpack(back_ref, target_ref, out_ref):
    rows = target_ref.shape[1]
    back = back_ref[...]
    target = target_ref[...]
    position = target % CAP
    value = jnp.broadcast_to(back[:, 0:1], (CLUSTERS, rows))
    for p in range(1, CAP):
        value = jnp.where(position == p, jnp.broadcast_to(back[:, p : p + 1], (CLUSTERS, rows)), value)
    member = iota((CLUSTERS, rows), 0) == target // CAP
    out_ref[...] = jnp.sum(jnp.where(member, value, 0.0), axis=0, keepdims=True)


def on_chip(x):
    return pltpu.with_memory_space_constraint(x, pltpu.VMEM)


def exchange(x):
    return lax.all_to_all(x, AXES, 0, 0, tiled=True)


def shards(embeddings, cluster_ids, ranks):
    rows, width = embeddings.shape
    slots = CLUSTERS * CAP
    wide = 2 * width + LANES
    f32, i32, bf16 = jnp.float32, jnp.int32, jnp.bfloat16
    shape = jax.ShapeDtypeStruct
    packed, target = pl.pallas_call(
        pack,
        out_shape=(pltpu.VMEM((CLUSTERS, 2, wide), bf16), pltpu.VMEM((1, rows), i32)),
        in_specs=[pl.BlockSpec(memory_space=pl.ANY)] * 3,
        out_specs=(VMEM, VMEM),
        scratch_shapes=[
            pltpu.VMEM((1, rows), i32),
            pltpu.VMEM((1, rows), i32),
            pltpu.VMEM((rows, width), bf16),
            pltpu.VMEM((rows, width), bf16),
            pltpu.VMEM((LANES, rows), bf16),
            pltpu.SemaphoreType.DMA((2 + CHUNKS,)),
        ],
        name="pack",
    )(cluster_ids.reshape(1, rows), ranks.reshape(1, rows), embeddings)
    arrived = exchange(packed)
    best = pl.pallas_call(
        score,
        out_shape=pltpu.VMEM((CLUSTERS, LANES), f32),
        in_specs=[VMEM],
        out_specs=VMEM,
        scratch_shapes=[pltpu.VMEM((slots, width), bf16), pltpu.VMEM((slots, LANES), f32)],
        name="score",
    )(on_chip(arrived))
    back = exchange(best.reshape(CLUSTERS, 1, LANES)).reshape(CLUSTERS, LANES)
    out = pl.pallas_call(
        unpack, out_shape=shape((1, rows), f32), in_specs=[VMEM, VMEM], name="unpack"
    )(on_chip(back), on_chip(target))
    return out.reshape(rows)


def solution(mesh):
    return jax.shard_map(
        shards,
        mesh=mesh,
        in_specs=(P(AXES, None), P(AXES, None), P(AXES)),
        out_specs=P(AXES),
        check_vma=False,
    )
```

```python
import jax
import jax.numpy as jnp
from jax import lax
from jax.experimental import pallas as pl
from jax.experimental.pallas import tpu as pltpu
from jax.sharding import Mesh, PartitionSpec as P

CLUSTERS = 256
CHIPS = 128
CAP = 4
LANES = 128
CHUNKS = 2
DIGIT = 64
DIGITS = 3
TILE = 256
FAR = (4, 2, 2)
AXES = "d"
VMEM = pl.BlockSpec(memory_space=pltpu.VMEM)
HBM = pl.BlockSpec(memory_space=pltpu.HBM)
LIMIT = pltpu.CompilerParams(vmem_limit_bytes=16 << 20)

epsilon = 1e-06


def flat(z, x, y, core):
    return ((z * 4 + x) * 2 + core) * 4 + y


def chip_order():
    chips = [(z, x, y) for z in range(8) for x in range(4) for y in range(4)]
    return [FAR] + [chip for chip in chips if chip != FAR]


CORES = [[flat(*chip, core) for chip in chip_order()] for core in range(2)]
PARTNER = [(flat(*chip, core), flat(*chip, 1 - core)) for chip in chip_order() for core in range(2)]


def this_core():
    return lax.axis_index(AXES) // 4 % 2


def iota(dims, dim):
    return lax.broadcasted_iota(jnp.int32, dims, dim)


def flag(mask):
    return mask.astype(jnp.float32).astype(jnp.bfloat16)


def dot(a, b, contract_b=0):
    return lax.dot_general(
        a, b, (((1,), (contract_b,)), ((), ())), preferred_element_type=jnp.float32
    )


def pack(ids_hbm, rank_hbm, rows_hbm, out_ref, target_ref, ids_ref, rank_ref, held, unit_ref, digit_ref, sems):
    rows, width = held.shape
    chunk = rows // CHUNKS
    loads = [
        pltpu.make_async_copy(ids_hbm, ids_ref, sems.at[0]),
        pltpu.make_async_copy(rank_hbm, rank_ref, sems.at[1]),
    ]
    for c in range(CHUNKS):
        part = pl.ds(c * chunk, chunk)
        loads.append(pltpu.make_async_copy(rows_hbm.at[part], held.at[part], sems.at[2 + c]))
    for load in loads:
        load.start()
    loads[0].wait()
    loads[1].wait()
    cluster = ids_ref[...]
    member = iota((CLUSTERS, rows), 0) == cluster
    before = iota((rows, rows), 0) < iota((rows, rows), 1)
    count = dot(flag(member), flag(before))
    position = jnp.sum(jnp.where(member, count, 0.0), axis=0, keepdims=True).astype(jnp.int32)
    chip, core = cluster // 2, cluster % 2
    other = jnp.where(core == this_core(), 0, 1)
    target_ref[...] = (chip * 2 + other) * CAP + position
    slot = ((other * 2 + position // 2) * CHIPS + chip) * 2 + position % 2
    rank = rank_ref[...] + 1
    which = iota((LANES, rows), 0) % DIGITS
    high, middle, low = rank // (DIGIT * DIGIT), rank // DIGIT % DIGIT, rank % DIGIT
    digits = jnp.where(which == 0, high, jnp.where(which == 1, middle, low))
    digit_ref[...] = digits.astype(jnp.float32).astype(jnp.bfloat16)
    for c in range(CHUNKS):
        loads[2 + c].wait()
        values = held[c * chunk : (c + 1) * chunk, :].astype(jnp.float32)
        scale = lax.rsqrt(jnp.sum(values * values, axis=1, keepdims=True) + epsilon)
        unit_ref[c * chunk : (c + 1) * chunk, :] = (values * scale).astype(jnp.bfloat16)
    pairs = 2 * CHIPS
    group = iota((pairs, LANES), 1) // DIGITS
    ranks = jnp.zeros((pairs, LANES), jnp.float32)
    for b in range(CAP):
        pick = flag(iota((pairs, rows), 0) + b * pairs == slot)
        packed = dot(pick, unit_ref[...]).astype(jnp.bfloat16)
        out_ref[:, :, b * width : (b + 1) * width] = packed.reshape(CHIPS, 2, width)
        ranks = jnp.where(group == b, dot(pick, digit_ref[...], 1), ranks)
    out_ref[:, :, CAP * width :] = ranks.astype(jnp.bfloat16).reshape(CHIPS, 2, LANES)


def hand(rows_ref, out_ref):
    chips, _, wide = rows_ref.shape
    pairs = 2 * chips
    width = (wide - LANES) // CAP
    for u in range(2):
        place = slice(u * pairs, (u + 1) * pairs)
        start = (2 + u) * width
        out_ref[place, :width] = rows_ref[:, :, start : start + width].reshape(pairs, width)
        out_ref[place, width:] = rows_ref[:, :, CAP * width :].reshape(pairs, LANES)


def weights(dims, dim, b):
    place = iota(dims, dim) - DIGITS * b
    value = jnp.where(place == 0, DIGIT * DIGIT, jnp.where(place == 1, DIGIT, jnp.where(place == 2, 1, 0)))
    return value.astype(jnp.float32).astype(jnp.bfloat16)


def settled(rank):
    return jnp.where(rank == 0.0, 1e9, rank)


def ranks_of(digits, b):
    down = settled(dot(digits, weights((LANES, LANES), 0, b)))
    return down, settled(dot(weights((8, LANES), 1, b), digits, 1))


def blocks_of(ref):
    return [ref[u * TILE : (u + 1) * TILE, :] for u in range(2)]


def raise_best(best, keys, down, across, pairs):
    parts = TILE // LANES
    diagonal = iota((LANES, LANES), 0) == iota((LANES, LANES), 1)
    for j in sorted({j for _, j in pairs}):
        top = [jnp.full((8, LANES), -1.0, jnp.float32)] * parts
        for i in [i for i, other in pairs if other == j]:
            scores = dot(keys[i], keys[j], 1)
            for part in range(parts):
                place = slice(part * LANES, (part + 1) * LANES)
                piece = scores[:, place]
                allowed = across[j][0:1, place] < down[i]
                best[i] = jnp.maximum(best[i], jnp.where(allowed, piece, -1.0))
                if i != j:
                    rest = jnp.where(allowed, -1.0, piece).reshape(TILE // 8, 8, LANES)
                    top[part] = jnp.maximum(top[part], jnp.max(rest, axis=0))
        extra = [jnp.where(diagonal, jnp.max(t, axis=0, keepdims=True), -1.0) for t in top]
        best[j] = jnp.maximum(best[j], jnp.concatenate(extra, axis=0))


def score_own(rows_ref, keys_ref, down_ref, across_ref, best_ref):
    _, _, wide = rows_ref.shape
    _, width = keys_ref.shape
    digits = rows_ref[:, :, CAP * width :].reshape(TILE, LANES)
    down, across = zip(*[ranks_of(digits, b) for b in range(2)])
    for u in range(2):
        place = slice(u * TILE, (u + 1) * TILE)
        keys_ref[place, :] = rows_ref[:, :, u * width : (u + 1) * width].reshape(TILE, width)
        down_ref[place, :] = down[u]
        across_ref[u * 8 : (u + 1) * 8, :] = across[u]
    best = [jnp.full((TILE, LANES), -1.0, jnp.float32)] * 2
    raise_best(best, blocks_of(keys_ref), down, across, [(0, 0), (0, 1), (1, 1)])
    for u in range(2):
        best_ref[u * TILE : (u + 1) * TILE, :] = best[u]


def score(own_ref, down_ref, across_ref, start_ref, got_ref, digit_ref, mine_ref, theirs_ref, best_ref):
    half, _ = own_ref.shape
    chips = half // CAP
    down, across = blocks_of(down_ref), [across_ref[u * 8 : (u + 1) * 8, :] for u in range(2)]
    for u, digits in enumerate(blocks_of(digit_ref)):
        column, row = ranks_of(digits, 2 + u)
        down.append(column)
        across.append(row)
    best = blocks_of(start_ref) + [jnp.full((TILE, LANES), -1.0, jnp.float32)] * 2
    pairs = [(0, 2), (1, 2), (2, 2), (0, 3), (1, 3), (2, 3), (3, 3)]
    raise_best(best, blocks_of(own_ref) + blocks_of(got_ref), down, across, pairs)
    for i in range(CAP):
        best_ref[i * TILE : (i + 1) * TILE, :] = jnp.broadcast_to(
            jnp.max(best[i], axis=1, keepdims=True), (TILE, LANES)
        )
    lane = iota((chips, LANES), 1)
    for other, ref in enumerate((mine_ref, theirs_ref)):
        out = jnp.full((chips, LANES), -jnp.inf, jnp.float32)
        for p in range(CAP):
            start = (2 * other + p // 2) * TILE + p % 2
            out = jnp.where(lane == CAP * other + p, best_ref[pl.ds(start, chips, stride=2), :], out)
        ref[...] = out


def unpack(back_ref, target_ref, out_ref):
    rows = target_ref.shape[1]
    back = back_ref[...]
    target = target_ref[...]
    place = target % (2 * CAP)
    value = jnp.zeros((CHIPS, rows), jnp.float32)
    for p in range(2 * CAP):
        value = jnp.where(place == p, jnp.broadcast_to(back[:, p : p + 1], (CHIPS, rows)), value)
    member = iota((CHIPS, rows), 0) == target // (2 * CAP)
    out_ref[...] = jnp.sum(jnp.where(member, value, 0.0), axis=0, keepdims=True)


def on_chip(x):
    return pltpu.with_memory_space_constraint(x, pltpu.VMEM)


def off_chip(x):
    return pltpu.with_memory_space_constraint(x, pltpu.HBM)


def exchange(x, groups):
    return lax.all_to_all(x, AXES, 0, 0, axis_index_groups=groups, tiled=True)


def swap(x):
    return lax.ppermute(x, AXES, PARTNER)


def shards(embeddings, cluster_ids, ranks):
    rows, width = embeddings.shape
    slots = CLUSTERS * CAP
    wide = CAP * width + LANES
    f32, i32, bf16 = jnp.float32, jnp.int32, jnp.bfloat16
    packed, target = pl.pallas_call(
        pack,
        out_shape=(pltpu.VMEM((CHIPS, 2, wide), bf16), pltpu.VMEM((1, rows), i32)),
        in_specs=[HBM] * 3,
        out_specs=(VMEM, VMEM),
        scratch_shapes=[
            pltpu.VMEM((1, rows), i32),
            pltpu.VMEM((1, rows), i32),
            pltpu.VMEM((rows, width), bf16),
            pltpu.VMEM((rows, width), bf16),
            pltpu.VMEM((LANES, rows), bf16),
            pltpu.SemaphoreType.DMA((2 + CHUNKS,)),
        ],
        compiler_params=LIMIT,
        name="pack",
    )(*map(off_chip, (cluster_ids.reshape(1, rows), ranks.reshape(1, rows), embeddings)))
    arrived = on_chip(exchange(packed, CORES))
    given = pl.pallas_call(
        hand,
        out_shape=pltpu.VMEM((slots // 2, width + LANES), bf16),
        in_specs=[VMEM],
        out_specs=VMEM,
        compiler_params=LIMIT,
        name="hand",
    )(arrived)
    with jax.named_scope("swap"):
        got = swap(given)
    half = slots // 2
    own, down, across, begun = pl.pallas_call(
        score_own,
        out_shape=(
            pltpu.VMEM((half, width), bf16),
            pltpu.VMEM((half, LANES), f32),
            pltpu.VMEM((16, TILE), f32),
            pltpu.VMEM((half, LANES), f32),
        ),
        in_specs=[VMEM],
        out_specs=(VMEM,) * 4,
        compiler_params=LIMIT,
        name="score_own",
    )(arrived)
    mine, theirs = pl.pallas_call(
        score,
        out_shape=(pltpu.VMEM((CHIPS, LANES), f32),) * 2,
        in_specs=[VMEM] * 6,
        out_specs=(VMEM, VMEM),
        scratch_shapes=[pltpu.VMEM((slots, LANES), f32)],
        compiler_params=LIMIT,
        name="score",
    )(*map(on_chip, (own, down, across, begun, got[:, :width], got[:, width:])))
    best = jnp.maximum(mine, swap(theirs))
    back = exchange(best.reshape(CHIPS, 1, LANES), CORES).reshape(CHIPS, LANES)
    out = pl.pallas_call(
        unpack,
        out_shape=jax.ShapeDtypeStruct((1, rows), f32),
        in_specs=[VMEM] * 2,
        compiler_params=LIMIT,
        name="unpack",
    )(*map(on_chip, (back, target)))
    return out.reshape(rows)


def solution(mesh):
    line = Mesh(mesh.devices.reshape(-1), (AXES,))
    return jax.shard_map(
        shards,
        mesh=line,
        in_specs=(P(AXES, None), P(AXES, None), P(AXES)),
        out_specs=P(AXES),
        check_vma=False,
    )
```

```python
import jax
import jax.numpy as jnp
from jax import lax
from jax.experimental import pallas as pl
from jax.experimental.pallas import tpu as pltpu
from jax.sharding import Mesh, PartitionSpec as P

CLUSTERS = 256
CHIPS = 128
CAP = 4
LANES = 128
CHUNKS = 2
DIGIT = 64
DIGITS = 3
TILE = 256
AXES = "d"
VMEM = pl.BlockSpec(memory_space=pltpu.VMEM)
HBM = pl.BlockSpec(memory_space=pltpu.HBM)
LIMIT = pltpu.CompilerParams(vmem_limit_bytes=16 << 20)

epsilon = 1e-06


def flat(z, x, y, core):
    return ((z * 4 + x) * 2 + core) * 4 + y


OUT_LEAD, BACK_LEAD = (5, 2, 3), (4, 2, 2)
CHIP_LIST = [(z, x, y) for z in range(8) for x in range(4) for y in range(4)]
OUT_CHIPS = [OUT_LEAD] + [chip for chip in CHIP_LIST if chip != OUT_LEAD]
LEAD = OUT_CHIPS.index(BACK_LEAD)
BACK_CHIPS = list(OUT_CHIPS)
BACK_CHIPS[0], BACK_CHIPS[LEAD] = OUT_CHIPS[LEAD], OUT_CHIPS[0]
OUT_GROUPS = [[flat(*chip, core) for chip in OUT_CHIPS] for core in range(2)]
BACK_GROUPS = [[flat(*chip, core) for chip in BACK_CHIPS] for core in range(2)]
PARTNER = [(flat(*chip, core), flat(*chip, 1 - core)) for chip in CHIP_LIST for core in range(2)]


def this_core():
    return lax.axis_index(AXES) // 4 % 2


def iota(dims, dim):
    return lax.broadcasted_iota(jnp.int32, dims, dim)


def flag(mask):
    return mask.astype(jnp.float32).astype(jnp.bfloat16)


def dot(a, b, contract_b=0):
    return lax.dot_general(
        a, b, (((1,), (contract_b,)), ((), ())), preferred_element_type=jnp.float32
    )


def pack(ids_hbm, rank_hbm, rows_hbm, out_ref, target_ref, ids_ref, rank_ref, held, unit_ref, digit_ref, sems):
    rows, width = held.shape
    chunk = rows // CHUNKS
    loads = [
        pltpu.make_async_copy(ids_hbm, ids_ref, sems.at[0]),
        pltpu.make_async_copy(rank_hbm, rank_ref, sems.at[1]),
    ]
    for c in range(CHUNKS):
        part = pl.ds(c * chunk, chunk)
        loads.append(pltpu.make_async_copy(rows_hbm.at[part], held.at[part], sems.at[2 + c]))
    for load in loads:
        load.start()
    loads[0].wait()
    loads[1].wait()
    cluster = ids_ref[...]
    member = iota((CLUSTERS, rows), 0) == cluster
    before = iota((rows, rows), 0) < iota((rows, rows), 1)
    count = dot(flag(member), flag(before))
    position = jnp.sum(jnp.where(member, count, 0.0), axis=0, keepdims=True).astype(jnp.int32)
    chip, core = cluster // 2, cluster % 2
    other = jnp.where(core == this_core(), 0, 1)
    back = jnp.where(chip == 0, LEAD, jnp.where(chip == LEAD, 0, chip))
    target_ref[...] = (back * 2 + other) * CAP + position
    slot = ((other * 2 + position // 2) * CHIPS + chip) * 2 + position % 2
    rank = rank_ref[...] + 1
    which = iota((LANES, rows), 0) % DIGITS
    high, middle, low = rank // (DIGIT * DIGIT), rank // DIGIT % DIGIT, rank % DIGIT
    digits = jnp.where(which == 0, high, jnp.where(which == 1, middle, low))
    digit_ref[...] = digits.astype(jnp.float32).astype(jnp.bfloat16)
    for c in range(CHUNKS):
        loads[2 + c].wait()
        values = held[c * chunk : (c + 1) * chunk, :].astype(jnp.float32)
        scale = lax.rsqrt(jnp.sum(values * values, axis=1, keepdims=True) + epsilon)
        unit_ref[c * chunk : (c + 1) * chunk, :] = (values * scale).astype(jnp.bfloat16)
    pairs = 2 * CHIPS
    group = iota((pairs, LANES), 1) // DIGITS
    ranks = jnp.zeros((pairs, LANES), jnp.float32)
    for b in range(CAP):
        pick = flag(iota((pairs, rows), 0) + b * pairs == slot)
        packed = dot(pick, unit_ref[...]).astype(jnp.bfloat16)
        out_ref[:, :, b * width : (b + 1) * width] = packed.reshape(CHIPS, 2, width)
        ranks = jnp.where(group == b, dot(pick, digit_ref[...], 1), ranks)
    out_ref[:, :, CAP * width :] = ranks.astype(jnp.bfloat16).reshape(CHIPS, 2, LANES)


def hand(rows_ref, out_ref):
    chips, _, wide = rows_ref.shape
    pairs = 2 * chips
    width = (wide - LANES) // CAP
    for u in range(2):
        place = slice(u * pairs, (u + 1) * pairs)
        start = (2 + u) * width
        out_ref[place, :width] = rows_ref[:, :, start : start + width].reshape(pairs, width)
        out_ref[place, width:] = rows_ref[:, :, CAP * width :].reshape(pairs, LANES)


def weights(dims, dim, b):
    place = iota(dims, dim) - DIGITS * b
    value = jnp.where(place == 0, DIGIT * DIGIT, jnp.where(place == 1, DIGIT, jnp.where(place == 2, 1, 0)))
    return value.astype(jnp.float32).astype(jnp.bfloat16)


def settled(rank):
    return jnp.where(rank == 0.0, 1e9, rank)


def ranks_of(digits, b):
    down = settled(dot(digits, weights((LANES, LANES), 0, b)))
    return down, settled(dot(weights((8, LANES), 1, b), digits, 1))


def blocks_of(ref):
    return [ref[u * TILE : (u + 1) * TILE, :] for u in range(2)]


def raise_best(best, keys, down, across, pairs):
    parts = TILE // LANES
    diagonal = iota((LANES, LANES), 0) == iota((LANES, LANES), 1)
    for j in sorted({j for _, j in pairs}):
        top = [jnp.full((8, LANES), -1.0, jnp.float32)] * parts
        for i in [i for i, other in pairs if other == j]:
            scores = dot(keys[i], keys[j], 1)
            for part in range(parts):
                place = slice(part * LANES, (part + 1) * LANES)
                piece = scores[:, place]
                allowed = across[j][0:1, place] < down[i]
                best[i] = jnp.maximum(best[i], jnp.where(allowed, piece, -1.0))
                if i != j:
                    rest = jnp.where(allowed, -1.0, piece).reshape(TILE // 8, 8, LANES)
                    top[part] = jnp.maximum(top[part], jnp.max(rest, axis=0))
        extra = [jnp.where(diagonal, jnp.max(t, axis=0, keepdims=True), -1.0) for t in top]
        best[j] = jnp.maximum(best[j], jnp.concatenate(extra, axis=0))


def gather_best(best, best_ref, first):
    for u in range(2):
        best_ref[u * TILE : (u + 1) * TILE, :] = jnp.broadcast_to(
            jnp.max(best[u], axis=1, keepdims=True), (TILE, LANES)
        )
    lane = iota((CHIPS, LANES), 1)
    out = jnp.full((CHIPS, LANES), -1.0, jnp.float32)
    for p in range(CAP):
        start = p // 2 * TILE + p % 2
        out = jnp.where(lane == first + p, best_ref[pl.ds(start, CHIPS, stride=2), :], out)
    return out


def score_here(rows_ref, given_ref, keys_ref, down_ref, begun_ref, out_ref, best_ref):
    _, _, wide = rows_ref.shape
    _, width = keys_ref.shape
    digits = rows_ref[:, :, CAP * width :].reshape(TILE, LANES)
    down, across = zip(*[ranks_of(digits, b) for b in range(CAP)])
    for u in range(2):
        place = slice(u * TILE, (u + 1) * TILE)
        keys_ref[place, :] = rows_ref[:, :, u * width : (u + 1) * width].reshape(TILE, width)
        down_ref[place, :] = down[u]
    keys = blocks_of(keys_ref) + [given_ref[u * TILE : (u + 1) * TILE, :width] for u in range(2)]
    best = [jnp.full((TILE, LANES), -1.0, jnp.float32)] * CAP
    raise_best(best, keys, down, across, [(0, 0), (0, 1), (1, 1)])
    for u in range(2):
        begun_ref[u * TILE : (u + 1) * TILE, :] = best[u]
    raise_best(best, keys, down, across, [(2, 2), (2, 3), (3, 3)])
    out_ref[...] = gather_best(best[2:], best_ref, CAP)


def score_swapped(keys_ref, down_ref, begun_ref, here_ref, got_ref, digit_ref, mine_ref, theirs_ref, best_ref):
    across = [None] * 2 + [ranks_of(digits, 2 + u)[1] for u, digits in enumerate(blocks_of(digit_ref))]
    best = blocks_of(begun_ref) + [jnp.full((TILE, LANES), -1.0, jnp.float32)] * 2
    pairs = [(0, 2), (1, 2), (0, 3), (1, 3)]
    raise_best(best, blocks_of(keys_ref) + blocks_of(got_ref), blocks_of(down_ref), across, pairs)
    mine = jnp.maximum(gather_best(best[:2], best_ref.at[0], 0), here_ref[...])
    for ref, found in ((mine_ref, mine), (theirs_ref, gather_best(best[2:], best_ref.at[1], CAP))):
        ref[...] = found
        ref[0:1, :] = found[LEAD : LEAD + 1, :]
        ref[LEAD : LEAD + 1, :] = found[0:1, :]


def unpack(back_ref, target_ref, out_ref):
    rows = target_ref.shape[1]
    back = back_ref[...]
    target = target_ref[...]
    place = target % (2 * CAP)
    value = jnp.zeros((CHIPS, rows), jnp.float32)
    for p in range(2 * CAP):
        value = jnp.where(place == p, jnp.broadcast_to(back[:, p : p + 1], (CHIPS, rows)), value)
    member = iota((CHIPS, rows), 0) == target // (2 * CAP)
    out_ref[...] = jnp.sum(jnp.where(member, value, 0.0), axis=0, keepdims=True)


def on_chip(x):
    return pltpu.with_memory_space_constraint(x, pltpu.VMEM)


def off_chip(x):
    return pltpu.with_memory_space_constraint(x, pltpu.HBM)


def exchange(x, groups):
    return lax.all_to_all(x, AXES, 0, 0, axis_index_groups=groups, tiled=True)


def swap(x):
    return lax.ppermute(x, AXES, PARTNER)


def shards(embeddings, cluster_ids, ranks):
    rows, width = embeddings.shape
    slots = CLUSTERS * CAP
    wide = CAP * width + LANES
    f32, i32, bf16 = jnp.float32, jnp.int32, jnp.bfloat16
    packed, target = pl.pallas_call(
        pack,
        out_shape=(pltpu.VMEM((CHIPS, 2, wide), bf16), pltpu.VMEM((1, rows), i32)),
        in_specs=[HBM] * 3,
        out_specs=(VMEM, VMEM),
        scratch_shapes=[
            pltpu.VMEM((1, rows), i32),
            pltpu.VMEM((1, rows), i32),
            pltpu.VMEM((rows, width), bf16),
            pltpu.VMEM((rows, width), bf16),
            pltpu.VMEM((LANES, rows), bf16),
            pltpu.SemaphoreType.DMA((2 + CHUNKS,)),
        ],
        compiler_params=LIMIT,
        name="pack",
    )(*map(off_chip, (cluster_ids.reshape(1, rows), ranks.reshape(1, rows), embeddings)))
    arrived = on_chip(exchange(packed, OUT_GROUPS))
    given = pl.pallas_call(
        hand,
        out_shape=pltpu.VMEM((slots // 2, width + LANES), bf16),
        in_specs=[VMEM],
        out_specs=VMEM,
        compiler_params=LIMIT,
        name="hand",
    )(arrived)
    with jax.named_scope("swap"):
        got = swap(given)
    half = slots // 2
    keys, down, begun, here = pl.pallas_call(
        score_here,
        out_shape=(
            pltpu.VMEM((half, width), bf16),
            pltpu.VMEM((half, LANES), f32),
            pltpu.VMEM((half, LANES), f32),
            pltpu.VMEM((CHIPS, LANES), f32),
        ),
        in_specs=[VMEM] * 2,
        out_specs=(VMEM,) * 4,
        scratch_shapes=[pltpu.VMEM((half, LANES), f32)],
        compiler_params=LIMIT,
        name="score_here",
    )(arrived, on_chip(given))
    mine, theirs = pl.pallas_call(
        score_swapped,
        out_shape=(pltpu.VMEM((CHIPS, LANES), f32),) * 2,
        in_specs=[VMEM] * 6,
        out_specs=(VMEM, VMEM),
        scratch_shapes=[pltpu.VMEM((2, half, LANES), f32)],
        compiler_params=LIMIT,
        name="score_swapped",
    )(*map(on_chip, (keys, down, begun, here, got[:, :width], got[:, width:])))
    best = jnp.maximum(mine, swap(theirs))
    back = exchange(best.reshape(CHIPS, 1, LANES), BACK_GROUPS).reshape(CHIPS, LANES)
    out = pl.pallas_call(
        unpack,
        out_shape=jax.ShapeDtypeStruct((1, rows), f32),
        in_specs=[VMEM] * 2,
        compiler_params=LIMIT,
        name="unpack",
    )(*map(on_chip, (back, target)))
    return out.reshape(rows)


def solution(mesh):
    line = Mesh(mesh.devices.reshape(-1), (AXES,))
    return jax.shard_map(
        shards,
        mesh=line,
        in_specs=(P(AXES, None), P(AXES, None), P(AXES)),
        out_specs=P(AXES),
        check_vma=False,
    )
```

```python
import jax
import jax.numpy as jnp
from jax import lax
from jax.experimental import pallas as pl
from jax.experimental.pallas import tpu as pltpu
from jax.sharding import Mesh, PartitionSpec as P

CLUSTERS = 256
CHIPS = 128
CAP = 4
LANES = 128
CHUNKS = 2
DIGIT = 64
DIGITS = 3
TILE = 256
AXES = "d"
VMEM = pl.BlockSpec(memory_space=pltpu.VMEM)
HBM = pl.BlockSpec(memory_space=pltpu.HBM)
LIMIT = pltpu.CompilerParams(vmem_limit_bytes=16 << 20)

epsilon = 1e-06


def flat(z, x, y, core):
    return ((z * 4 + x) * 2 + core) * 4 + y


OUT_LEAD, BACK_LEAD = (5, 2, 3), (4, 2, 2)
CHIP_LIST = [(z, x, y) for z in range(8) for x in range(4) for y in range(4)]
OUT_CHIPS = [OUT_LEAD] + [chip for chip in CHIP_LIST if chip != OUT_LEAD]
LEAD = OUT_CHIPS.index(BACK_LEAD)
BACK_CHIPS = list(OUT_CHIPS)
BACK_CHIPS[0], BACK_CHIPS[LEAD] = OUT_CHIPS[LEAD], OUT_CHIPS[0]
OUT_GROUPS = [[flat(*chip, core) for chip in OUT_CHIPS] for core in range(2)]
BACK_GROUPS = [[flat(*chip, core) for chip in BACK_CHIPS] for core in range(2)]
PARTNER = [(flat(*chip, core), flat(*chip, 1 - core)) for chip in CHIP_LIST for core in range(2)]


def this_core():
    return lax.axis_index(AXES) // 4 % 2


def iota(dims, dim):
    return lax.broadcasted_iota(jnp.int32, dims, dim)


def flag(mask):
    return mask.astype(jnp.float32).astype(jnp.bfloat16)


def dot(a, b, contract_b=0):
    return lax.dot_general(
        a, b, (((1,), (contract_b,)), ((), ())), preferred_element_type=jnp.float32
    )


def pack(ids_hbm, rank_hbm, rows_hbm, out_ref, target_ref, ids_ref, rank_ref, held, unit_ref, digit_ref, sems):
    rows, width = held.shape
    chunk = rows // CHUNKS
    loads = [
        pltpu.make_async_copy(ids_hbm, ids_ref, sems.at[0]),
        pltpu.make_async_copy(rank_hbm, rank_ref, sems.at[1]),
    ]
    for c in range(CHUNKS):
        part = pl.ds(c * chunk, chunk)
        loads.append(pltpu.make_async_copy(rows_hbm.at[part], held.at[part], sems.at[2 + c]))
    for load in loads:
        load.start()
    loads[0].wait()
    loads[1].wait()
    cluster = ids_ref[...]
    member = iota((CLUSTERS, rows), 0) == cluster
    before = iota((rows, rows), 0) < iota((rows, rows), 1)
    count = dot(flag(member), flag(before))
    position = jnp.sum(jnp.where(member, count, 0.0), axis=0, keepdims=True).astype(jnp.int32)
    chip, core = cluster // 2, cluster % 2
    other = jnp.where(core == this_core(), 0, 1)
    back = jnp.where(chip == 0, LEAD, jnp.where(chip == LEAD, 0, chip))
    target_ref[...] = (back * 2 + other) * CAP + position
    slot = ((other * 2 + position // 2) * CHIPS + chip) * 2 + position % 2
    rank = rank_ref[...] + 1
    which = iota((LANES, rows), 0) % DIGITS
    high, middle, low = rank // (DIGIT * DIGIT), rank // DIGIT % DIGIT, rank % DIGIT
    digits = jnp.where(which == 0, high, jnp.where(which == 1, middle, low))
    digit_ref[...] = digits.astype(jnp.float32).astype(jnp.bfloat16)
    for c in range(CHUNKS):
        loads[2 + c].wait()
        values = held[c * chunk : (c + 1) * chunk, :].astype(jnp.float32)
        scale = lax.rsqrt(jnp.sum(values * values, axis=1, keepdims=True) + epsilon)
        unit_ref[c * chunk : (c + 1) * chunk, :] = (values * scale).astype(jnp.bfloat16)
    pairs = 2 * CHIPS
    group = iota((pairs, LANES), 1) // DIGITS
    pick = flag(iota((CAP * pairs, rows), 0) == slot)
    packed = dot(pick, unit_ref[...]).astype(jnp.bfloat16)
    digits = dot(pick, digit_ref[...], 1)
    ranks = jnp.zeros((pairs, LANES), jnp.float32)
    for b in range(CAP):
        out_ref[:, :, b * width : (b + 1) * width] = packed[b * pairs : (b + 1) * pairs].reshape(CHIPS, 2, width)
        ranks = jnp.where(group == b, digits[b * pairs : (b + 1) * pairs], ranks)
    out_ref[:, :, CAP * width :] = ranks.astype(jnp.bfloat16).reshape(CHIPS, 2, LANES)


def hand(rows_ref, out_ref):
    chips, _, wide = rows_ref.shape
    pairs = 2 * chips
    width = (wide - LANES) // CAP
    for u in range(2):
        place = slice(u * pairs, (u + 1) * pairs)
        start = (2 + u) * width
        out_ref[place, :width] = rows_ref[:, :, start : start + width].reshape(pairs, width)
        out_ref[place, width:] = rows_ref[:, :, CAP * width :].reshape(pairs, LANES)


def weights(dims, dim, b):
    place = iota(dims, dim) - DIGITS * b
    value = jnp.where(place == 0, DIGIT * DIGIT, jnp.where(place == 1, DIGIT, jnp.where(place == 2, 1, 0)))
    return value.astype(jnp.float32).astype(jnp.bfloat16)


def settled(rank):
    return jnp.where(rank == 0.0, 1e9, rank)


def ranks_of(digits, b):
    down = settled(dot(digits, weights((LANES, LANES), 0, b)))
    return down, settled(dot(weights((8, LANES), 1, b), digits, 1))


def blocks_of(ref):
    return [ref[u * TILE : (u + 1) * TILE, :] for u in range(2)]


def raise_best(best, keys, down, across, pairs):
    parts = TILE // LANES
    diagonal = iota((LANES, LANES), 0) == iota((LANES, LANES), 1)
    for j in sorted({j for _, j in pairs}):
        top = [jnp.full((8, LANES), -1.0, jnp.float32)] * parts
        for i in [i for i, other in pairs if other == j]:
            scores = dot(keys[i], keys[j], 1)
            for part in range(parts):
                place = slice(part * LANES, (part + 1) * LANES)
                piece = scores[:, place]
                allowed = across[j][0:1, place] < down[i]
                best[i] = jnp.maximum(best[i], jnp.where(allowed, piece, -1.0))
                if i != j:
                    rest = jnp.where(allowed, -1.0, piece).reshape(TILE // 8, 8, LANES)
                    top[part] = jnp.maximum(top[part], jnp.max(rest, axis=0))
        extra = [jnp.where(diagonal, jnp.max(t, axis=0, keepdims=True), -1.0) for t in top]
        best[j] = jnp.maximum(best[j], jnp.concatenate(extra, axis=0))


def gather_best(best, best_ref, first):
    for u in range(2):
        best_ref[u * TILE : (u + 1) * TILE, :] = jnp.broadcast_to(
            jnp.max(best[u], axis=1, keepdims=True), (TILE, LANES)
        )
    lane = iota((CHIPS, LANES), 1)
    out = jnp.full((CHIPS, LANES), -1.0, jnp.float32)
    for p in range(CAP):
        start = p // 2 * TILE + p % 2
        out = jnp.where(lane == first + p, best_ref[pl.ds(start, CHIPS, stride=2), :], out)
    return out


def score_here(rows_ref, given_ref, keys_ref, down_ref, begun_ref, out_ref, best_ref):
    _, _, wide = rows_ref.shape
    _, width = keys_ref.shape
    digits = rows_ref[:, :, CAP * width :].reshape(TILE, LANES)
    down, across = zip(*[ranks_of(digits, b) for b in range(CAP)])
    for u in range(2):
        place = slice(u * TILE, (u + 1) * TILE)
        keys_ref[place, :] = rows_ref[:, :, u * width : (u + 1) * width].reshape(TILE, width)
        down_ref[place, :] = down[u]
    keys = blocks_of(keys_ref) + [given_ref[u * TILE : (u + 1) * TILE, :width] for u in range(2)]
    best = [jnp.full((TILE, LANES), -1.0, jnp.float32)] * CAP
    raise_best(best, keys, down, across, [(0, 0), (0, 1), (1, 1)])
    for u in range(2):
        begun_ref[u * TILE : (u + 1) * TILE, :] = best[u]
    raise_best(best, keys, down, across, [(2, 2), (2, 3), (3, 3)])
    out_ref[...] = gather_best(best[2:], best_ref, CAP)


def score_swapped(keys_ref, down_ref, begun_ref, here_ref, got_ref, digit_ref, mine_ref, theirs_ref, best_ref):
    across = [None] * 2 + [ranks_of(digits, 2 + u)[1] for u, digits in enumerate(blocks_of(digit_ref))]
    best = blocks_of(begun_ref) + [jnp.full((TILE, LANES), -1.0, jnp.float32)] * 2
    pairs = [(0, 2), (1, 2), (0, 3), (1, 3)]
    raise_best(best, blocks_of(keys_ref) + blocks_of(got_ref), blocks_of(down_ref), across, pairs)
    mine = jnp.maximum(gather_best(best[:2], best_ref.at[0], 0), here_ref[...])
    for ref, found in ((mine_ref, mine), (theirs_ref, gather_best(best[2:], best_ref.at[1], CAP))):
        ref[...] = found
        ref[0:1, :] = found[LEAD : LEAD + 1, :]
        ref[LEAD : LEAD + 1, :] = found[0:1, :]


def unpack(back_ref, target_ref, out_ref):
    rows = target_ref.shape[1]
    back = back_ref[...]
    target = target_ref[...]
    place = target % (2 * CAP)
    value = jnp.zeros((CHIPS, rows), jnp.float32)
    for p in range(2 * CAP):
        value = jnp.where(place == p, jnp.broadcast_to(back[:, p : p + 1], (CHIPS, rows)), value)
    member = iota((CHIPS, rows), 0) == target // (2 * CAP)
    out_ref[...] = jnp.sum(jnp.where(member, value, 0.0), axis=0, keepdims=True)


def on_chip(x):
    return pltpu.with_memory_space_constraint(x, pltpu.VMEM)


def off_chip(x):
    return pltpu.with_memory_space_constraint(x, pltpu.HBM)


def exchange(x, groups):
    return lax.all_to_all(x, AXES, 0, 0, axis_index_groups=groups, tiled=True)


def swap(x):
    return lax.ppermute(x, AXES, PARTNER)


def shards(embeddings, cluster_ids, ranks):
    rows, width = embeddings.shape
    slots = CLUSTERS * CAP
    wide = CAP * width + LANES
    f32, i32, bf16 = jnp.float32, jnp.int32, jnp.bfloat16
    packed, target = pl.pallas_call(
        pack,
        out_shape=(pltpu.VMEM((CHIPS, 2, wide), bf16), pltpu.VMEM((1, rows), i32)),
        in_specs=[HBM] * 3,
        out_specs=(VMEM, VMEM),
        scratch_shapes=[
            pltpu.VMEM((1, rows), i32),
            pltpu.VMEM((1, rows), i32),
            pltpu.VMEM((rows, width), bf16),
            pltpu.VMEM((rows, width), bf16),
            pltpu.VMEM((LANES, rows), bf16),
            pltpu.SemaphoreType.DMA((2 + CHUNKS,)),
        ],
        compiler_params=LIMIT,
        name="pack",
    )(*map(off_chip, (cluster_ids.reshape(1, rows), ranks.reshape(1, rows), embeddings)))
    arrived = on_chip(exchange(packed, OUT_GROUPS))
    given = pl.pallas_call(
        hand,
        out_shape=pltpu.VMEM((slots // 2, width + LANES), bf16),
        in_specs=[VMEM],
        out_specs=VMEM,
        compiler_params=LIMIT,
        name="hand",
    )(arrived)
    with jax.named_scope("swap"):
        got = swap(given)
    half = slots // 2
    keys, down, begun, here = pl.pallas_call(
        score_here,
        out_shape=(
            pltpu.VMEM((half, width), bf16),
            pltpu.VMEM((half, LANES), f32),
            pltpu.VMEM((half, LANES), f32),
            pltpu.VMEM((CHIPS, LANES), f32),
        ),
        in_specs=[VMEM] * 2,
        out_specs=(VMEM,) * 4,
        scratch_shapes=[pltpu.VMEM((half, LANES), f32)],
        compiler_params=LIMIT,
        name="score_here",
    )(arrived, on_chip(given))
    mine, theirs = pl.pallas_call(
        score_swapped,
        out_shape=(pltpu.VMEM((CHIPS, LANES), f32),) * 2,
        in_specs=[VMEM] * 6,
        out_specs=(VMEM, VMEM),
        scratch_shapes=[pltpu.VMEM((2, half, LANES), f32)],
        compiler_params=LIMIT,
        name="score_swapped",
    )(*map(on_chip, (keys, down, begun, here, got[:, :width], got[:, width:])))
    best = jnp.maximum(mine, swap(theirs))
    back = exchange(best.reshape(CHIPS, 1, LANES), BACK_GROUPS).reshape(CHIPS, LANES)
    out = pl.pallas_call(
        unpack,
        out_shape=jax.ShapeDtypeStruct((1, rows), f32),
        in_specs=[VMEM] * 2,
        compiler_params=LIMIT,
        name="unpack",
    )(*map(on_chip, (back, target)))
    return out.reshape(rows)


def solution(mesh):
    line = Mesh(mesh.devices.reshape(-1), (AXES,))
    return jax.shard_map(
        shards,
        mesh=line,
        in_specs=(P(AXES, None), P(AXES, None), P(AXES)),
        out_specs=P(AXES),
        check_vma=False,
    )
```

```python
import jax
import jax.numpy as jnp
from jax import lax
from jax.experimental import pallas as pl
from jax.experimental.pallas import tpu as pltpu
from jax.sharding import Mesh, PartitionSpec as P

CLUSTERS = 256
CHIPS = 128
CAP = 4
LANES = 128
CHUNKS = 2
DIGIT = 64
DIGITS = 3
TILE = 256
AXES = "d"
VMEM = pl.BlockSpec(memory_space=pltpu.VMEM)
HBM = pl.BlockSpec(memory_space=pltpu.HBM)
LIMIT = pltpu.CompilerParams(vmem_limit_bytes=16 << 20)

epsilon = 1e-06


def flat(z, x, y, core):
    return ((z * 4 + x) * 2 + core) * 4 + y


OUT_LEAD, BACK_LEAD = (5, 2, 3), (4, 2, 2)
CHIP_LIST = [(z, x, y) for z in range(8) for x in range(4) for y in range(4)]
OUT_CHIPS = [OUT_LEAD] + [chip for chip in CHIP_LIST if chip != OUT_LEAD]
LEAD = OUT_CHIPS.index(BACK_LEAD)
BACK_CHIPS = list(OUT_CHIPS)
BACK_CHIPS[0], BACK_CHIPS[LEAD] = OUT_CHIPS[LEAD], OUT_CHIPS[0]
OUT_GROUPS = [[flat(*chip, core) for chip in OUT_CHIPS] for core in range(2)]
BACK_GROUPS = [[flat(*chip, core) for chip in BACK_CHIPS] for core in range(2)]
PARTNER = [(flat(*chip, core), flat(*chip, 1 - core)) for chip in CHIP_LIST for core in range(2)]


def this_core():
    return lax.axis_index(AXES) // 4 % 2


def iota(dims, dim):
    return lax.broadcasted_iota(jnp.int32, dims, dim)


def flag(mask):
    return mask.astype(jnp.float32).astype(jnp.bfloat16)


def dot(a, b, contract_b=0):
    return lax.dot_general(
        a, b, (((1,), (contract_b,)), ((), ())), preferred_element_type=jnp.float32
    )


def pack(ids_hbm, rank_hbm, rows_hbm, out_ref, target_ref, ids_ref, rank_ref, held, unit_ref, digit_ref, sems):
    rows, width = held.shape
    chunk = rows // CHUNKS
    loads = [
        pltpu.make_async_copy(ids_hbm, ids_ref, sems.at[0]),
        pltpu.make_async_copy(rank_hbm, rank_ref, sems.at[1]),
    ]
    for c in range(CHUNKS):
        part = pl.ds(c * chunk, chunk)
        loads.append(pltpu.make_async_copy(rows_hbm.at[part], held.at[part], sems.at[2 + c]))
    for load in loads:
        load.start()
    loads[0].wait()
    loads[1].wait()
    cluster = ids_ref[...]
    member = iota((CLUSTERS, rows), 0) == cluster
    before = iota((rows, rows), 0) < iota((rows, rows), 1)
    count = dot(flag(member), flag(before))
    position = jnp.sum(jnp.where(member, count, 0.0), axis=0, keepdims=True).astype(jnp.int32)
    chip, core = cluster // 2, cluster % 2
    other = jnp.where(core == this_core(), 0, 1)
    back = jnp.where(chip == 0, LEAD, jnp.where(chip == LEAD, 0, chip))
    target_ref[...] = (back * 2 + other) * CAP + position
    slot = ((other * 2 + position // 2) * CHIPS + chip) * 2 + position % 2
    rank = rank_ref[...] + 1
    which = iota((LANES, rows), 0) % DIGITS
    high, middle, low = rank // (DIGIT * DIGIT), rank // DIGIT % DIGIT, rank % DIGIT
    digits = jnp.where(which == 0, high, jnp.where(which == 1, middle, low))
    digit_ref[...] = digits.astype(jnp.float32).astype(jnp.bfloat16)
    for c in range(CHUNKS):
        loads[2 + c].wait()
        values = held[c * chunk : (c + 1) * chunk, :].astype(jnp.float32)
        scale = lax.rsqrt(jnp.sum(values * values, axis=1, keepdims=True) + epsilon)
        unit_ref[c * chunk : (c + 1) * chunk, :] = (values * scale).astype(jnp.bfloat16)
    pairs = 2 * CHIPS
    group = iota((pairs, LANES), 1) // DIGITS
    pick = flag(iota((CAP * pairs, rows), 0) == slot)
    packed = dot(pick, unit_ref[...]).astype(jnp.bfloat16)
    digits = dot(pick, digit_ref[...], 1)
    ranks = jnp.zeros((pairs, LANES), jnp.float32)
    for b in range(CAP):
        out_ref[:, :, b * width : (b + 1) * width] = packed[b * pairs : (b + 1) * pairs].reshape(CHIPS, 2, width)
        ranks = jnp.where(group == b, digits[b * pairs : (b + 1) * pairs], ranks)
    out_ref[:, :, CAP * width :] = ranks.astype(jnp.bfloat16).reshape(CHIPS, 2, LANES)


def hand(rows_ref, *out_refs):
    _, _, wide = rows_ref.shape
    width = (wide - LANES) // CAP
    for u, ref in enumerate(out_refs):
        start = (2 + u) * width
        ref[:, :width] = rows_ref[:, :, start : start + width].reshape(TILE, width)
        ref[:, width:] = rows_ref[:, :, CAP * width :].reshape(TILE, LANES)


def weights(dims, dim, b):
    place = iota(dims, dim) - DIGITS * b
    value = jnp.where(place == 0, DIGIT * DIGIT, jnp.where(place == 1, DIGIT, jnp.where(place == 2, 1, 0)))
    return value.astype(jnp.float32).astype(jnp.bfloat16)


def settled(rank):
    return jnp.where(rank == 0.0, 1e9, rank)


def ranks_of(digits, b):
    down = settled(dot(digits, weights((LANES, LANES), 0, b)))
    return down, settled(dot(weights((8, LANES), 1, b), digits, 1))


def blocks_of(ref):
    return [ref[u * TILE : (u + 1) * TILE, :] for u in range(2)]


def raise_best(best, keys, down, across, pairs):
    parts = TILE // LANES
    diagonal = iota((LANES, LANES), 0) == iota((LANES, LANES), 1)
    for j in sorted({j for _, j in pairs}):
        top = [jnp.full((8, LANES), -1.0, jnp.float32)] * parts
        for i in [i for i, other in pairs if other == j]:
            scores = dot(keys[i], keys[j], 1)
            for part in range(parts):
                place = slice(part * LANES, (part + 1) * LANES)
                piece = scores[:, place]
                allowed = across[j][0:1, place] < down[i]
                best[i] = jnp.maximum(best[i], jnp.where(allowed, piece, -1.0))
                if i != j:
                    rest = jnp.where(allowed, -1.0, piece).reshape(TILE // 8, 8, LANES)
                    top[part] = jnp.maximum(top[part], jnp.max(rest, axis=0))
        extra = [jnp.where(diagonal, jnp.max(t, axis=0, keepdims=True), -1.0) for t in top]
        best[j] = jnp.maximum(best[j], jnp.concatenate(extra, axis=0))


def gather_best(best, best_ref, first):
    for u in range(2):
        best_ref[u * TILE : (u + 1) * TILE, :] = jnp.broadcast_to(
            jnp.max(best[u], axis=1, keepdims=True), (TILE, LANES)
        )
    lane = iota((CHIPS, LANES), 1)
    out = jnp.full((CHIPS, LANES), -1.0, jnp.float32)
    for p in range(CAP):
        start = p // 2 * TILE + p % 2
        out = jnp.where(lane == first + p, best_ref[pl.ds(start, CHIPS, stride=2), :], out)
    return out


def score_here(rows_ref, first_ref, second_ref, keys_ref, down_ref, begun_ref, out_ref, best_ref):
    _, _, wide = rows_ref.shape
    _, width = keys_ref.shape
    digits = rows_ref[:, :, CAP * width :].reshape(TILE, LANES)
    down, across = zip(*[ranks_of(digits, b) for b in range(CAP)])
    for u in range(2):
        place = slice(u * TILE, (u + 1) * TILE)
        keys_ref[place, :] = rows_ref[:, :, u * width : (u + 1) * width].reshape(TILE, width)
        down_ref[place, :] = down[u]
    keys = blocks_of(keys_ref) + [ref[:, :width] for ref in (first_ref, second_ref)]
    best = [jnp.full((TILE, LANES), -1.0, jnp.float32)] * CAP
    raise_best(best, keys, down, across, [(0, 0), (0, 1), (1, 1)])
    for u in range(2):
        begun_ref[u * TILE : (u + 1) * TILE, :] = best[u]
    raise_best(best, keys, down, across, [(2, 2), (2, 3), (3, 3)])
    out_ref[...] = gather_best(best[2:], best_ref, CAP)


def score_first(keys_ref, down_ref, begun_ref, got_ref, digit_ref, raised_ref):
    across = [None] * 2 + [ranks_of(digit_ref[...], 2)[1]]
    best = blocks_of(begun_ref) + [jnp.full((TILE, LANES), -1.0, jnp.float32)]
    raise_best(best, blocks_of(keys_ref) + [got_ref[...]], blocks_of(down_ref), across, [(0, 2), (1, 2)])
    for u in range(3):
        raised_ref[u * TILE : (u + 1) * TILE, :] = best[u]


def put(ref, found):
    ref[...] = found
    ref[0:1, :] = found[LEAD : LEAD + 1, :]
    ref[LEAD : LEAD + 1, :] = found[0:1, :]


def score_second(keys_ref, down_ref, raised_ref, got_ref, digit_ref, final_ref, theirs_ref, best_ref):
    across = [None] * 2 + [ranks_of(digit_ref[...], 3)[1]]
    best = blocks_of(raised_ref) + [jnp.full((TILE, LANES), -1.0, jnp.float32)]
    raise_best(best, blocks_of(keys_ref) + [got_ref[...]], blocks_of(down_ref), across, [(0, 2), (1, 2)])
    put(theirs_ref, gather_best([raised_ref[2 * TILE :, :], best[2]], best_ref, CAP))
    for u in range(2):
        final_ref[u * TILE : (u + 1) * TILE, :] = best[u]


def settle(final_ref, here_ref, mine_ref, best_ref):
    put(mine_ref, jnp.maximum(gather_best(blocks_of(final_ref), best_ref, 0), here_ref[...]))


def unpack(back_ref, target_ref, out_ref):
    rows = target_ref.shape[1]
    back = back_ref[...]
    target = target_ref[...]
    place = target % (2 * CAP)
    value = jnp.zeros((CHIPS, rows), jnp.float32)
    for p in range(2 * CAP):
        value = jnp.where(place == p, jnp.broadcast_to(back[:, p : p + 1], (CHIPS, rows)), value)
    member = iota((CHIPS, rows), 0) == target // (2 * CAP)
    out_ref[...] = jnp.sum(jnp.where(member, value, 0.0), axis=0, keepdims=True)


def on_chip(x):
    return pltpu.with_memory_space_constraint(x, pltpu.VMEM)


def off_chip(x):
    return pltpu.with_memory_space_constraint(x, pltpu.HBM)


def exchange(x, groups):
    return lax.all_to_all(x, AXES, 0, 0, axis_index_groups=groups, tiled=True)


def swap(x):
    return lax.ppermute(x, AXES, PARTNER)


def shards(embeddings, cluster_ids, ranks):
    rows, width = embeddings.shape
    slots = CLUSTERS * CAP
    wide = CAP * width + LANES
    f32, i32, bf16 = jnp.float32, jnp.int32, jnp.bfloat16
    packed, target = pl.pallas_call(
        pack,
        out_shape=(pltpu.VMEM((CHIPS, 2, wide), bf16), pltpu.VMEM((1, rows), i32)),
        in_specs=[HBM] * 3,
        out_specs=(VMEM, VMEM),
        scratch_shapes=[
            pltpu.VMEM((1, rows), i32),
            pltpu.VMEM((1, rows), i32),
            pltpu.VMEM((rows, width), bf16),
            pltpu.VMEM((rows, width), bf16),
            pltpu.VMEM((LANES, rows), bf16),
            pltpu.SemaphoreType.DMA((2 + CHUNKS,)),
        ],
        compiler_params=LIMIT,
        name="pack",
    )(*map(off_chip, (cluster_ids.reshape(1, rows), ranks.reshape(1, rows), embeddings)))
    arrived = on_chip(exchange(packed, OUT_GROUPS))
    half = slots // 2
    given = pl.pallas_call(
        hand,
        out_shape=(pltpu.VMEM((TILE, width + LANES), bf16),) * 2,
        in_specs=[VMEM],
        out_specs=(VMEM,) * 2,
        compiler_params=LIMIT,
        name="hand",
    )(arrived)
    got = [swap(part) for part in given]
    keys, down, begun, here = pl.pallas_call(
        score_here,
        out_shape=(
            pltpu.VMEM((half, width), bf16),
            pltpu.VMEM((half, LANES), f32),
            pltpu.VMEM((half, LANES), f32),
            pltpu.VMEM((CHIPS, LANES), f32),
        ),
        in_specs=[VMEM] * 3,
        out_specs=(VMEM,) * 4,
        scratch_shapes=[pltpu.VMEM((half, LANES), f32)],
        compiler_params=LIMIT,
        name="score_here",
    )(arrived, *map(on_chip, given))
    raised = pl.pallas_call(
        score_first,
        out_shape=pltpu.VMEM((3 * TILE, LANES), f32),
        in_specs=[VMEM] * 5,
        out_specs=VMEM,
        compiler_params=LIMIT,
        name="score_first",
    )(*map(on_chip, (keys, down, begun, got[0][:, :width], got[0][:, width:])))
    final, theirs = pl.pallas_call(
        score_second,
        out_shape=(pltpu.VMEM((half, LANES), f32), pltpu.VMEM((CHIPS, LANES), f32)),
        in_specs=[VMEM] * 5,
        out_specs=(VMEM, VMEM),
        scratch_shapes=[pltpu.VMEM((half, LANES), f32)],
        compiler_params=LIMIT,
        name="score_second",
    )(*map(on_chip, (keys, down, raised, got[1][:, :width], got[1][:, width:])))
    mine = pl.pallas_call(
        settle,
        out_shape=pltpu.VMEM((CHIPS, LANES), f32),
        in_specs=[VMEM] * 2,
        out_specs=VMEM,
        scratch_shapes=[pltpu.VMEM((half, LANES), f32)],
        compiler_params=LIMIT,
        name="settle",
    )(on_chip(final), on_chip(here))
    best = jnp.maximum(mine, swap(theirs))
    back = exchange(best.reshape(CHIPS, 1, LANES), BACK_GROUPS).reshape(CHIPS, LANES)
    out = pl.pallas_call(
        unpack,
        out_shape=jax.ShapeDtypeStruct((1, rows), f32),
        in_specs=[VMEM] * 2,
        compiler_params=LIMIT,
        name="unpack",
    )(*map(on_chip, (back, target)))
    return out.reshape(rows)


def solution(mesh):
    line = Mesh(mesh.devices.reshape(-1), (AXES,))
    return jax.shard_map(
        shards,
        mesh=line,
        in_specs=(P(AXES, None), P(AXES, None), P(AXES)),
        out_specs=P(AXES),
        check_vma=False,
    )
```
